32 devices in a mesh: dp: 4 (over x, core), section: 2 (over y), mp: 4 (over z).
Axes of the slice: x: 2, y: 2, z: 4, core: 2. Of those that a mesh axis runs over, the one named last changes fastest.
Arguments:
- micro_inputs: bfloat16 [8, 64, 4096], P(('dp', 'section'), None, 'mp'), parts along dimension 0, may hold values from -6 to 6
- qkv_weight: bfloat16 [2, 4096, 3, 2048], P('section', None, None, 'mp'), may hold values from -0.09375 to 0.09375
- out_weight: bfloat16 [2, 2048, 4096], P('section', None, 'mp'), may hold values from -0.125 to 0.125
- norm_gain: bfloat16 [2, 4096], P('section'), may hold values from 0.099609375 to 1.8984375
- position_bias: float32 [32, 32], P('mp'), may hold values from -3 to 280
Outputs:
- encoded: bfloat16 [8, 64, 4096], P(('dp', 'section'), None, 'mp'), parts along dimension 0
The draws below stay inside these ranges and needn't reach their ends.
There are 4 independent parts, one for each index of `dp`. The reference program is written for one: setup_inputs(seed, part) draws one part's arguments, and reference() takes and returns one part's arrays. A program takes and returns all parts, laid end to end along the dimension named above; an argument that names none is the same for every part. Nothing has to cross between parts.
All inputs are finite; a program needn't handle non-finite values.
Results may differ from the reference program's by a relative error of at most 0.025.
Values may be sent and summed in bfloat16 or wider, within the bound.
A program may use at most 128 MiB of HBM per device.

```python
import math
import jax
import jax.numpy as jnp
import numpy as np
from jax import lax

D = 4096
HS = 64
HEADS = 32
BUCKETS = 32
REACH = 128
LENGTH = 64
LAYERS = 2
MICROS = 2


def draw_position_bias(key, part):
    ordinary = jnp.clip(jax.random.normal(key, (HEADS, BUCKETS), jnp.float32), -3.0, 3.0)
    return ordinary


def shard_levels(rng, dims, shards, smallest, largest):
    def one(position, parts):
        steps = jax.random.uniform(jax.random.fold_in(jax.random.fold_in(rng, 6), position), (parts,), jnp.float32, smallest / len(shards), largest / len(shards))
        return jnp.repeat(jnp.exp(steps), dims[position] // parts).reshape((-1,) + (1,) * (len(dims) - position - 1))

    level = one(*shards[0])
    for cut in shards[1:]:
        level = level * one(*cut)
    return level


def centred(rng, shape, scale, most, split=(), kind=jnp.bfloat16):
    values = scale * jax.random.normal(rng, shape, jnp.float32)
    if split:
        values = values * shard_levels(rng, shape, split, -0.22, 0.18)
    return jnp.clip(values, -most, most).astype(kind)


def setup_inputs(seed: int = 0, part: int = 0) -> dict:
    seeds = jax.random.split(jax.random.key(seed), 6)
    own_keys = jax.random.split(jax.random.fold_in(seeds[5], part), 6)
    micro_inputs = centred(own_keys[0], (MICROS, LENGTH, D), 1.0, 6.0, ((0, 2), (2, 4)))
    qkv_weight = centred(seeds[1], (LAYERS, D, 3, HEADS * HS), D ** -0.5, 0.09375, ((0, 2), (3, 4)))
    out_weight = centred(seeds[2], (LAYERS, HEADS * HS, D), (HEADS * HS) ** -0.5, 0.125, ((0, 2), (2, 4)))
    norm_gain = jnp.clip(1.0 + 0.18 * jax.random.normal(seeds[3], (LAYERS, D), jnp.float32), 0.099609375, 1.8984375).astype(jnp.bfloat16)
    position_bias = draw_position_bias(jax.random.fold_in(seeds[5], 71), part)
    return {"micro_inputs": micro_inputs, "qkv_weight": qkv_weight, "out_weight": out_weight, "norm_gain": norm_gain, "position_bias": position_bias}


NORM_EPSILON = 0.1

def bucket_table(length, bucket_count, reach_limit):
    offset = np.arange(length)[None, :] - np.arange(length)[:, None]
    half_count = bucket_count // 2
    upper_side = (offset > 0).astype(np.int32) * half_count
    distance = np.abs(offset)
    exact_count = half_count // 2
    scaled = np.log(np.maximum(distance, 1) / exact_count) / np.log(reach_limit / exact_count) * (half_count - exact_count)
    far_bucket = np.minimum(exact_count + scaled.astype(np.int32), half_count - 1)
    return (upper_side + np.where(distance < exact_count, distance, far_bucket)).astype(np.int32)

def reference(micro_inputs, qkv_weight, out_weight, norm_gain, position_bias):
    bucket_grid = jnp.asarray(bucket_table(LENGTH, BUCKETS, REACH)).astype(jnp.int32)
    score_bias = position_bias[:, bucket_grid].astype(jnp.float32)
    score_scale = 1.0 / math.sqrt(HS)

    def layer_step(hidden, layer_index):
        stream = hidden.astype(jnp.float32)
        mean_square = lax.optimization_barrier(jnp.mean(stream * stream, axis=1, keepdims=True))
        row_scale = lax.rsqrt(mean_square + NORM_EPSILON)
        gained = (stream * norm_gain[layer_index].astype(jnp.float32)).astype(jnp.bfloat16)
        weight_grid = qkv_weight[layer_index].reshape(D, 3 * HEADS * HS)
        project = jnp.dot(gained, weight_grid, preferred_element_type=jnp.float32) * row_scale
        rounded = lax.optimization_barrier(project.astype(jnp.bfloat16))
        project = rounded.astype(jnp.float32).reshape(LENGTH, 3, HEADS, HS)
        queries = project[:, 0]
        key_heads = project[:, 1]
        values = project[:, 2]
        scores = jnp.einsum('ihd,jhd->hij', queries, key_heads, precision=lax.Precision.HIGHEST) * score_scale + score_bias
        row_max = lax.optimization_barrier(jnp.max(scores, axis=2, keepdims=True))
        weights = jnp.exp(scores - row_max)
        attn_probs = lax.optimization_barrier((weights / lax.optimization_barrier(jnp.sum(weights, axis=2, keepdims=True))).astype(jnp.bfloat16))
        head_mix = jnp.einsum('hij,jhd->ihd', attn_probs.astype(jnp.float32), values, precision=lax.Precision.HIGHEST)
        head_mix = head_mix.astype(jnp.bfloat16).reshape(LENGTH, HEADS * HS)
        update = jnp.dot(head_mix, out_weight[layer_index], preferred_element_type=jnp.float32)
        return ((stream + update).astype(jnp.bfloat16), None)

    def run_micro(micro_rows):
        finished, unused = lax.scan(layer_step, micro_rows, jnp.arange(LAYERS, dtype=jnp.int32))
        return finished
    return lax.map(run_micro, micro_inputs)
```

```python
import functools
import math

import jax
import jax.numpy as jnp
import numpy as np
from jax import lax
from jax.experimental import pallas as pl
from jax.experimental.pallas import tpu as pltpu
from jax.sharding import PartitionSpec as P

REACH = 128
NORM_EPSILON = 0.1
MESH = pl.DeviceIdType.MESH
LAST_DETOUR = 3
EARLY = 1


def bucket_table(length, bucket_count, reach_limit):
    offset = np.arange(length)[None, :] - np.arange(length)[:, None]
    half_count = bucket_count // 2
    upper_side = (offset > 0).astype(np.int32) * half_count
    distance = np.abs(offset)
    exact_count = half_count // 2
    scaled = (
        np.log(np.maximum(distance, 1) / exact_count)
        / np.log(reach_limit / exact_count)
        * (half_count - exact_count)
    )
    far_bucket = np.minimum(exact_count + scaled.astype(np.int32), half_count - 1)
    return (upper_side + np.where(distance < exact_count, distance, far_bucket)).astype(np.int32)


def head_group(heads, head_size):
    return max(g for g in range(1, heads + 1) if heads % g == 0 and g * head_size <= 256)


def column_parts(width):
    return 2 if width % 256 == 0 else 1


def kernel(
    sizes,
    x_ref, gain_ref, bucket_ref, pbias_ref, wq_hbm, wo_hbm,
    o_ref,
    xg, hg, transit, ho, fin, wq, wo, acc, out_acc, sq, qkv, bias, head_mask,
    wq_sem, wo_sem,
    x_recv, line_send, first_send, up_send, straight_send, relay_send,
    mix_recv, mix_send, transit_recv, transit_up, transit_send,
    fin_send, fin_recv,
):
    S, M, L, H, hs = sizes
    C, _, Dc = ho.shape
    _, parts, _, Wp = transit.shape
    Dl = x_ref.shape[1]
    Wl = H * hs
    G = head_group(H, hs)
    Wg = G * hs
    D = M * Dl
    s = lax.axis_index("section")
    m = lax.axis_index("mp")

    def to(src, dst, send, recv, sec, col):
        return pltpu.make_async_remote_copy(
            src_ref=src, dst_ref=dst, send_sem=send, recv_sem=recv,
            device_id={"section": sec, "mp": col}, device_id_type=MESH,
        )

    def start(c):
        c.start()

    def sent(c):
        c.wait_send()

    def got(dst, recv):
        to(dst, dst, fin_send.at[0], recv, s, lax.rem(m + 1, M)).wait_recv()

    near = jnp.minimum(m, M - 1 - m)
    longer = jnp.where(m > M - 1 - m, -1, 1)

    def nth(p):
        k = (p + 1) // 2
        both = jnp.where(p % 2 == 1, -k, k)
        return m + jnp.where(p <= 2 * near, both, longer * (p - near))

    def others(body):
        def step(p, carry):
            j = nth(p)
            body(j, jnp.abs(j - m))
            return carry

        lax.fori_loop(1, M, step, 0)

    def others_far_first(body):
        def step(p, carry):
            j = nth(M - p)
            body(j, jnp.abs(j - m))
            return carry

        lax.fori_loop(1, M, step, 0)

    def wq_copy(j):
        rows = pl.ds(pl.multiple_of(j * Dl, Dl), Dl)
        return pltpu.make_async_copy(wq_hbm.at[:, rows, :], wq.at[:, rows, :], wq_sem.at[j])

    def wo_copy():
        return pltpu.make_async_copy(wo_hbm, wo, wo_sem)

    barrier = pltpu.get_barrier_semaphore()
    for o in range(S):
        for k in range(M):
            if o or k:
                pl.semaphore_signal(
                    barrier, inc=1,
                    device_id={"section": lax.rem(s + o, S), "mp": lax.rem(m + k, M)},
                    device_id_type=MESH,
                )

    for p in range(M):
        wq_copy(nth(p)).start()
    wo_copy().start()
    pl.semaphore_wait(barrier, S * M - 1)

    def rows_of(i):
        return pl.ds(i * L, L)

    def x_part(c):
        return x_ref.at[:, pl.ds(c * Dc, Dc)]

    def block(i, c, j):
        return xg.at[j, c, rows_of(i), :]

    def along(j, c, src, act):
        dst = block(0, c, j)
        even = lax.rem(m - j + 2 * M, 2) == 0
        for reach in (2, 1):
            @pl.when((j <= m) & even & (m < M - reach))
            def _():
                act(to(src, dst, line_send.at[c, reach - 1, j], x_recv.at[0, c, j], s, m + reach))

            @pl.when((j >= m) & even & (m >= reach))
            def _():
                act(to(src, dst, line_send.at[c, reach + 1, j], x_recv.at[0, c, j], s, m - reach))

    def first_out(act):
        def one(i, c, j):
            dst = xg.at[m, c, pl.ds(pl.multiple_of(i * L, L), L), :]
            act(to(x_part(c), dst, first_send.at[c, j], x_recv.at[i, c, m], 0, j))

        for c in range(C):
            one(s, c, m)
            others_far_first(lambda j, d: one(s, c, j))

    @pl.when(s == 0)
    def _():
        for c in range(C):
            along(m, c, x_part(c), start)

    @pl.when(s > 0)
    def _():
        first_out(start)

    for g in range(H // G):
        heads = []
        for h in range(g * G, (g + 1) * G):
            total = jnp.zeros(bucket_ref.shape, jnp.float32)
            for b in range(pbias_ref.shape[1]):
                total = jnp.where(bucket_ref[...] == b, pbias_ref[h, b], total)
            heads.append(total)
        bias[g] = jnp.concatenate(heads, axis=1)
    head_mask[...] = jnp.where(
        lax.broadcasted_iota(jnp.int32, (G * L, Wg), 0) // L
        == lax.broadcasted_iota(jnp.int32, (G * L, Wg), 1) // hs,
        1.0,
        0.0,
    ).astype(jnp.bfloat16)

    pair = s + 1 - 2 * lax.rem(s, 2)
    paired = pair < S

    def detour_from(i, row):
        return jnp.where((lax.rem(row, 2) == 1) & (i == S - 1), LAST_DETOUR, 3)

    def detoured(i, row, d):
        return paired & (d >= detour_from(i, row))

    def mix_part(i, g, j):
        return hg.at[rows_of(i), pl.ds(pl.multiple_of(j * Wl + g * Wp, Wp), Wp)]

    def far_reach(i, row):
        return paired & (jnp.maximum(m, M - 1 - m) >= detour_from(i, row))

    def mix_act(i, g, act):
        src = mix_part(i, g, m)

        @pl.when(far_reach(i, s))
        def _():
            act(to(src, transit.at[i, g], transit_up.at[i, g], transit_recv.at[i, g], pair, m))

        def one(j, d):
            @pl.when(jnp.logical_not(detoured(i, s, d)))
            def _():
                act(to(src, src, mix_send.at[i, g, j], mix_recv.at[i, g, m], s, j))

        others_far_first(one)

    def transit_act(i, g, act):
        def one(j, d):
            @pl.when(detoured(i, pair, d))
            def _():
                act(to(transit.at[i, g], mix_part(i, g, m), transit_send.at[i, g, j],
                       mix_recv.at[i, g, m], pair, j))

        others(one)

    def transit_all(act, wait):
        for i in range(S):
            @pl.when(far_reach(i, pair))
            def _():
                for g in range(parts):
                    if wait:
                        got(transit.at[i, g], transit_recv.at[i, g])
                    transit_act(i, g, act)

    def relay_act(i, c, act):
        def one(j, d):
            @pl.when(lax.rem(d, 2) == 1)
            def _():
                act(to(block(i, c, m), block(i, c, m), relay_send.at[i, c, j], x_recv.at[i, c, m], s, j))

        others_far_first(one)

    def relay(i):
        for c in range(C):
            got(block(i, c, m), x_recv.at[i, c, m])
            relay_act(i, c, start)

    @pl.when(lax.rem(s, 2) == 1)
    def _():
        transit_all(start, True)

    scale = 1.0 / math.sqrt(hs)
    lane_head = lax.broadcasted_iota(jnp.int32, (L, Wg), 1) // hs

    def attend(i):
        for g in range(H // G):
            q = qkv[:, g * Wg : (g + 1) * Wg]
            k = qkv[:, Wl + g * Wg : Wl + (g + 1) * Wg]
            v = qkv[:, 2 * Wl + g * Wg : 2 * Wl + (g + 1) * Wg]
            apart = jnp.concatenate([q] * G, axis=0) * head_mask[...]
            scores = lax.dot_general(
                k, apart, (((1,), (1,)), ((), ())), preferred_element_type=jnp.float32
            ) * scale + bias[g]
            weights = jnp.exp(scores - jnp.max(scores, axis=0, keepdims=True))
            probs = (weights / jnp.sum(weights, axis=0, keepdims=True)).astype(jnp.bfloat16)
            mixed = lax.dot_general(
                probs, v, (((0,), (0,)), ((), ())), preferred_element_type=jnp.float32
            )
            out = mixed[0:L]
            for h in range(1, G):
                out = jnp.where(lane_head == h, mixed[h * L : (h + 1) * L], out)
            cols = pl.ds(pl.multiple_of(m * Wl + g * Wg, Wg), Wg)
            hg[i * L : (i + 1) * L, cols] = out.astype(jnp.bfloat16)
            if parts > 1:
                mix_act(i, g, start)
        if parts == 1:
            mix_act(i, 0, start)

    def qkv_block(i, c, j):
        part_block = xg[j, c, i * L : (i + 1) * L, :].astype(jnp.float32)
        squares = part_block * part_block
        part = squares[:, 0:128]
        for k in range(1, Dc // 128):
            part = part + squares[:, k * 128 : (k + 1) * 128]
        sq[...] += part
        rows = pl.ds(pl.multiple_of(j * Dl + c * Dc, Dc), Dc)
        gained = (part_block * gain_ref[:, rows].astype(jnp.float32)).astype(jnp.bfloat16)
        for t in range(3):
            cols = pl.ds(t * Wl, Wl)
            acc[:, cols] += jnp.dot(gained, wq[t, rows, :], preferred_element_type=jnp.float32)

    for i in range(S):
        acc[...] = jnp.zeros_like(acc)
        sq[...] = jnp.zeros_like(sq)

        if i == 0:
            @pl.when(s == 0)
            def _():
                for c in range(C):
                    xg[m, c, 0:L, :] = x_ref[:, c * Dc : (c + 1) * Dc]

            @pl.when(s > 0)
            def _():
                relay(0)

        def qkv_step(p, carry):
            j = nth(p)
            if i == 0:
                wq_copy(j).wait()
            for c in range(C):
                @pl.when((j != m) | (s == 0) & (i > 0))
                def _():
                    got(block(i, c, j), x_recv.at[i, c, j])
                    if i == 0:
                        @pl.when(s == 0)
                        def _():
                            along(j, c, block(0, c, j), start)
                qkv_block(i, c, j)
            return carry

        early = min(EARLY, M)
        lax.fori_loop(0, early, qkv_step, 0)
        if i < S - 1:
            @pl.when(s > 0)
            def _():
                relay(i + 1)
        lax.fori_loop(early, M, qkv_step, 0)
        row_scale = lax.rsqrt(jnp.sum(sq[...], axis=1, keepdims=True) / D + NORM_EPSILON)
        qkv[...] = (acc[...] * row_scale).astype(jnp.bfloat16)
        attend(i)

    wo_copy().wait()

    def ho_part(i, c):
        return ho.at[c, rows_of(i), :]

    def up_act(i, c, act):
        act(to(ho_part(i, c), block(i, c, m), up_send.at[i, c], x_recv.at[i, c, m], s + 1, m))

    def straight_act(i, c, act):
        def one(j, d):
            @pl.when(lax.rem(d, 2) == 0)
            def _():
                act(to(ho_part(i, c), block(i, c, m), straight_send.at[i, c, j], x_recv.at[i, c, m], s + 1, j))

        others_far_first(one)

    def home(i, act):
        act(to(ho.at[:, rows_of(i), :], fin, fin_send.at[i], fin_recv, i, m))

    for i in range(S):
        def out_step(p, carry):
            j = nth(p)

            @pl.when(j != m)
            def _():
                for g in range(parts):
                    got(mix_part(i, g, j), mix_recv.at[i, g, j])
            cols = pl.ds(pl.multiple_of(j * Wl, Wl), Wl)
            update = jnp.dot(hg[i * L : (i + 1) * L, cols], wo[cols, :], preferred_element_type=jnp.float32)
            out_acc[...] = jnp.where(p == 0, update, out_acc[...] + update)
            return carry

        lax.fori_loop(0, M, out_step, 0)
        for c in range(C):
            total = xg[m, c, i * L : (i + 1) * L, :].astype(jnp.float32) + out_acc[:, c * Dc : (c + 1) * Dc]
            ho[c, i * L : (i + 1) * L, :] = total.astype(jnp.bfloat16)

            @pl.when(s < S - 1)
            def _():
                up_act(i, c, start)

        @pl.when(s < S - 1)
        def _():
            for c in range(C):
                straight_act(i, c, start)

        if i < S - 1:
            @pl.when(s == S - 1)
            def _():
                home(i, start)

    @pl.when(lax.rem(s, 2) == 0)
    def _():
        transit_all(start, True)

    @pl.when(s == 0)
    def _():
        for c in range(C):
            along(m, c, x_part(c), sent)
            others(lambda j, d: along(j, c, block(0, c, j), sent))

    @pl.when(s > 0)
    def _():
        first_out(sent)

    for i in range(S):
        for g in range(parts):
            mix_act(i, g, sent)

        @pl.when(s > 0)
        def _():
            for c in range(C):
                relay_act(i, c, sent)

        @pl.when(s < S - 1)
        def _():
            for c in range(C):
                up_act(i, c, sent)
                straight_act(i, c, sent)

        if i < S - 1:
            @pl.when(s == S - 1)
            def _():
                home(i, sent)

    transit_all(sent, False)

    @pl.when(s == S - 1)
    def _():
        for c in range(C):
            o_ref[:, c * Dc : (c + 1) * Dc] = ho[c, (S - 1) * L :, :]

    @pl.when(s < S - 1)
    def _():
        got(fin, fin_recv)
        for c in range(C):
            o_ref[:, c * Dc : (c + 1) * Dc] = fin[c]


def solution(mesh):
    S, M = mesh.shape["section"], mesh.shape["mp"]

    def shards(micro_inputs, qkv_weight, out_weight, norm_gain, position_bias):
        L, Dl = micro_inputs.shape[1:]
        D = qkv_weight.shape[1]
        Wl = qkv_weight.shape[3]
        H = position_bias.shape[0]
        R = S * L
        hs = Wl // H
        G = head_group(H, hs)
        N = H // G
        parts = N
        C = column_parts(Dl)
        buckets = jnp.asarray(bucket_table(L, position_bias.shape[1], REACH).T)
        wq = jnp.transpose(qkv_weight[0], (1, 0, 2))
        bf16, f32 = jnp.bfloat16, jnp.float32
        dma = pltpu.SemaphoreType.DMA
        vmem = pl.BlockSpec(memory_space=pltpu.VMEM)
        out = pl.pallas_call(
            functools.partial(kernel, (S, M, L, H, hs)),
            out_shape=pltpu.VMEM((L, Dl), bf16),
            in_specs=[
                vmem, vmem, vmem, pl.BlockSpec(memory_space=pltpu.SMEM),
                pl.BlockSpec(memory_space=pltpu.HBM), pl.BlockSpec(memory_space=pltpu.HBM),
            ],
            out_specs=vmem,
            scratch_shapes=[
                pltpu.VMEM((M, C, R, Dl // C), bf16),
                pltpu.VMEM((R, M * Wl), bf16),
                pltpu.VMEM((S, parts, L, Wl // parts), bf16),
                pltpu.VMEM((C, R, Dl // C), bf16),
                pltpu.VMEM((C, L, Dl // C), bf16),
                pltpu.VMEM((3, D, Wl), bf16),
                pltpu.VMEM((M * Wl, Dl), bf16),
                pltpu.VMEM((L, 3 * Wl), f32),
                pltpu.VMEM((L, Dl), f32),
                pltpu.VMEM((L, 128), f32),
                pltpu.VMEM((L, 3 * Wl), bf16),
                pltpu.VMEM((N, L, G * L), f32),
                pltpu.VMEM((G * L, G * hs), bf16),
                dma((M,)), dma,
                dma((S, C, M)), dma((C, 4, M)), dma((C, M)), dma((S, C)), dma((S, C, M)), dma((S, C, M)),
                dma((S, parts, M)), dma((S, parts, M)), dma((S, parts)), dma((S, parts)), dma((S, parts, M)),
                dma((S,)), dma,
            ],
            compiler_params=pltpu.CompilerParams(
                collective_id=0, has_side_effects=True, vmem_limit_bytes=60 * 1024 * 1024
            ),
        )(micro_inputs[0], norm_gain, buckets, position_bias, wq, out_weight[0])
        return out[None]

    in_specs = (
        P(("dp", "section"), None, "mp"),
        P("section", None, None, "mp"),
        P("section", None, "mp"),
        P("section", None),
        P("mp", None),
    )
    out_specs = P(("dp", "section"), None, "mp")
    return jax.shard_map(shards, mesh=mesh, in_specs=in_specs, out_specs=out_specs, check_vma=False)
```

```python
import functools
import math

import jax
import jax.numpy as jnp
import numpy as np
from jax import lax
from jax.experimental import pallas as pl
from jax.experimental.pallas import tpu as pltpu
from jax.sharding import PartitionSpec as P

REACH = 128
NORM_EPSILON = 0.1
MESH = pl.DeviceIdType.MESH
LAST_DETOUR = 3
EARLY = 1


def bucket_table(length, bucket_count, reach_limit):
    offset = np.arange(length)[None, :] - np.arange(length)[:, None]
    half_count = bucket_count // 2
    upper_side = (offset > 0).astype(np.int32) * half_count
    distance = np.abs(offset)
    exact_count = half_count // 2
    scaled = (
        np.log(np.maximum(distance, 1) / exact_count)
        / np.log(reach_limit / exact_count)
        * (half_count - exact_count)
    )
    far_bucket = np.minimum(exact_count + scaled.astype(np.int32), half_count - 1)
    return (upper_side + np.where(distance < exact_count, distance, far_bucket)).astype(np.int32)


def head_group(heads, head_size):
    return max(g for g in range(1, heads + 1) if heads % g == 0 and g * head_size <= 256)


def column_parts(width):
    return 2 if width % 256 == 0 else 1


def kernel(
    sizes,
    x_ref, gain_ref, bucket_ref, pbias_ref, wq_hbm, wo_hbm,
    o_ref,
    xg, hg, transit, ho, fin, wq, wo, acc, out_acc, sq, qkv, bias, head_mask,
    wq_sem, wo_sem,
    x_recv, line_send, first_send, up_send, straight_send, relay_send,
    mix_recv, mix_send, transit_recv, transit_up, transit_send,
    fin_send, fin_recv,
):
    S, M, L, H, hs = sizes
    C, _, Dc = ho.shape
    _, parts, _, Wp = transit.shape
    Dl = x_ref.shape[1]
    Wl = H * hs
    G = head_group(H, hs)
    Wg = G * hs
    D = M * Dl
    s = lax.axis_index("section")
    m = lax.axis_index("mp")

    def to(src, dst, send, recv, sec, col):
        return pltpu.make_async_remote_copy(
            src_ref=src, dst_ref=dst, send_sem=send, recv_sem=recv,
            device_id={"section": sec, "mp": col}, device_id_type=MESH,
        )

    def start(c):
        c.start()

    def sent(c):
        c.wait_send()

    def got(dst, recv):
        to(dst, dst, fin_send.at[0], recv, s, lax.rem(m + 1, M)).wait_recv()

    near = jnp.minimum(m, M - 1 - m)
    longer = jnp.where(m > M - 1 - m, -1, 1)

    def nth(p):
        k = (p + 1) // 2
        both = jnp.where(p % 2 == 1, -k, k)
        return m + jnp.where(p <= 2 * near, both, longer * (p - near))

    hand_on = jnp.where(near > 0, 3, 2) if M > 3 else 1

    def relay_first(p):
        return nth(jnp.where(p == 1, hand_on, jnp.where((p > 1) & (p <= hand_on), p - 1, p)))

    def others(body):
        def step(p, carry):
            j = nth(p)
            body(j, jnp.abs(j - m))
            return carry

        lax.fori_loop(1, M, step, 0)

    def others_far_first(body):
        def step(p, carry):
            j = nth(M - p)
            body(j, jnp.abs(j - m))
            return carry

        lax.fori_loop(1, M, step, 0)

    def wq_copy(j):
        rows = pl.ds(pl.multiple_of(j * Dl, Dl), Dl)
        return pltpu.make_async_copy(wq_hbm.at[:, rows, :], wq.at[:, rows, :], wq_sem.at[j])

    def wo_copy():
        return pltpu.make_async_copy(wo_hbm, wo, wo_sem)

    barrier = pltpu.get_barrier_semaphore()
    for o in range(S):
        for k in range(M):
            if o or k:
                pl.semaphore_signal(
                    barrier, inc=1,
                    device_id={"section": lax.rem(s + o, S), "mp": lax.rem(m + k, M)},
                    device_id_type=MESH,
                )

    for p in range(M):
        wq_copy(nth(p)).start()
    wo_copy().start()
    pl.semaphore_wait(barrier, S * M - 1)

    def rows_of(i):
        return pl.ds(i * L, L)

    def x_part(c):
        return x_ref.at[:, pl.ds(c * Dc, Dc)]

    def block(i, c, j):
        return xg.at[j, c, rows_of(i), :]

    def along(j, c, src, act):
        dst = block(0, c, j)
        even = lax.rem(m - j + 2 * M, 2) == 0
        for reach in (2, 1):
            @pl.when((j <= m) & even & (m < M - reach))
            def _():
                act(to(src, dst, line_send.at[c, reach - 1, j], x_recv.at[0, c, j], s, m + reach))

            @pl.when((j >= m) & even & (m >= reach))
            def _():
                act(to(src, dst, line_send.at[c, reach + 1, j], x_recv.at[0, c, j], s, m - reach))

    def first_out(act):
        def one(i, c, j):
            dst = xg.at[m, c, pl.ds(pl.multiple_of(i * L, L), L), :]
            act(to(x_part(c), dst, first_send.at[c, j], x_recv.at[i, c, m], 0, j))

        for c in range(C):
            one(s, c, m)
            others_far_first(lambda j, d: one(s, c, j))

    @pl.when(s == 0)
    def _():
        for c in range(C):
            along(m, c, x_part(c), start)

    @pl.when(s > 0)
    def _():
        first_out(start)

    for g in range(H // G):
        heads = []
        for h in range(g * G, (g + 1) * G):
            total = jnp.zeros(bucket_ref.shape, jnp.float32)
            for b in range(pbias_ref.shape[1]):
                total = jnp.where(bucket_ref[...] == b, pbias_ref[h, b], total)
            heads.append(total)
        bias[g] = jnp.concatenate(heads, axis=1)
    head_mask[...] = jnp.where(
        lax.broadcasted_iota(jnp.int32, (G * L, Wg), 0) // L
        == lax.broadcasted_iota(jnp.int32, (G * L, Wg), 1) // hs,
        1.0,
        0.0,
    ).astype(jnp.bfloat16)

    pair = s + 1 - 2 * lax.rem(s, 2)
    paired = pair < S

    def detour_from(i, row):
        return jnp.where((lax.rem(row, 2) == 1) & (i == S - 1), LAST_DETOUR, 3)

    def detoured(i, row, d):
        return paired & (d >= detour_from(i, row))

    def mix_part(i, g, j):
        return hg.at[rows_of(i), pl.ds(pl.multiple_of(j * Wl + g * Wp, Wp), Wp)]

    def far_reach(i, row):
        return paired & (jnp.maximum(m, M - 1 - m) >= detour_from(i, row))

    def mix_act(i, g, act):
        src = mix_part(i, g, m)

        @pl.when(far_reach(i, s))
        def _():
            act(to(src, transit.at[i, g], transit_up.at[i, g], transit_recv.at[i, g], pair, m))

        def one(j, d):
            @pl.when(jnp.logical_not(detoured(i, s, d)))
            def _():
                act(to(src, src, mix_send.at[i, g, j], mix_recv.at[i, g, m], s, j))

        others_far_first(one)

    def transit_act(i, g, act):
        def one(j, d):
            @pl.when(detoured(i, pair, d))
            def _():
                act(to(transit.at[i, g], mix_part(i, g, m), transit_send.at[i, g, j],
                       mix_recv.at[i, g, m], pair, j))

        others(one)

    def transit_all(act, wait):
        for i in range(S):
            @pl.when(far_reach(i, pair))
            def _():
                for g in range(parts):
                    if wait:
                        got(transit.at[i, g], transit_recv.at[i, g])
                    transit_act(i, g, act)

    def relay_act(i, c, act):
        def one(j, d):
            @pl.when(lax.rem(d, 2) == 1)
            def _():
                act(to(block(i, c, m), block(i, c, m), relay_send.at[i, c, j], x_recv.at[i, c, m], s, j))

        others_far_first(one)

    def relay(i):
        for c in range(C):
            got(block(i, c, m), x_recv.at[i, c, m])
            relay_act(i, c, start)

    @pl.when(lax.rem(s, 2) == 1)
    def _():
        transit_all(start, True)

    scale = 1.0 / math.sqrt(hs)
    lane_head = lax.broadcasted_iota(jnp.int32, (L, Wg), 1) // hs

    def attend(i):
        for g in range(H // G):
            q = qkv[:, g * Wg : (g + 1) * Wg]
            k = qkv[:, Wl + g * Wg : Wl + (g + 1) * Wg]
            v = qkv[:, 2 * Wl + g * Wg : 2 * Wl + (g + 1) * Wg]
            apart = jnp.concatenate([q] * G, axis=0) * head_mask[...]
            scores = lax.dot_general(
                k, apart, (((1,), (1,)), ((), ())), preferred_element_type=jnp.float32
            ) * scale + bias[g]
            weights = jnp.exp(scores - jnp.max(scores, axis=0, keepdims=True))
            probs = (weights / jnp.sum(weights, axis=0, keepdims=True)).astype(jnp.bfloat16)
            mixed = lax.dot_general(
                probs, v, (((0,), (0,)), ((), ())), preferred_element_type=jnp.float32
            )
            out = mixed[0:L]
            for h in range(1, G):
                out = jnp.where(lane_head == h, mixed[h * L : (h + 1) * L], out)
            cols = pl.ds(pl.multiple_of(m * Wl + g * Wg, Wg), Wg)
            hg[i * L : (i + 1) * L, cols] = out.astype(jnp.bfloat16)
            if parts > 1:
                mix_act(i, g, start)
        if parts == 1:
            mix_act(i, 0, start)

    def qkv_block(i, c, j):
        part_block = xg[j, c, i * L : (i + 1) * L, :].astype(jnp.float32)
        squares = part_block * part_block
        part = squares[:, 0:128]
        for k in range(1, Dc // 128):
            part = part + squares[:, k * 128 : (k + 1) * 128]
        sq[...] += part
        rows = pl.ds(pl.multiple_of(j * Dl + c * Dc, Dc), Dc)
        gained = (part_block * gain_ref[:, rows].astype(jnp.float32)).astype(jnp.bfloat16)
        for t in range(3):
            cols = pl.ds(t * Wl, Wl)
            acc[:, cols] += jnp.dot(gained, wq[t, rows, :], preferred_element_type=jnp.float32)

    for i in range(S):
        acc[...] = jnp.zeros_like(acc)
        sq[...] = jnp.zeros_like(sq)

        if i == 0:
            @pl.when(s == 0)
            def _():
                for c in range(C):
                    xg[m, c, 0:L, :] = x_ref[:, c * Dc : (c + 1) * Dc]

            @pl.when(s > 0)
            def _():
                relay(0)

        def qkv_step(p, carry):
            j = jnp.where(s == 0, relay_first(p), nth(p)) if i == 0 else nth(p)
            if i == 0:
                wq_copy(j).wait()
            for c in range(C):
                @pl.when((j != m) | (s == 0) & (i > 0))
                def _():
                    got(block(i, c, j), x_recv.at[i, c, j])
                    if i == 0:
                        @pl.when(s == 0)
                        def _():
                            along(j, c, block(0, c, j), start)
                qkv_block(i, c, j)
            return carry

        early = min(EARLY, M)
        lax.fori_loop(0, early, qkv_step, 0)
        if i < S - 1:
            @pl.when(s > 0)
            def _():
                relay(i + 1)
        lax.fori_loop(early, M, qkv_step, 0)
        row_scale = lax.rsqrt(jnp.sum(sq[...], axis=1, keepdims=True) / D + NORM_EPSILON)
        qkv[...] = (acc[...] * row_scale).astype(jnp.bfloat16)
        attend(i)

    wo_copy().wait()

    def ho_part(i, c):
        return ho.at[c, rows_of(i), :]

    def up_act(i, c, act):
        act(to(ho_part(i, c), block(i, c, m), up_send.at[i, c], x_recv.at[i, c, m], s + 1, m))

    def straight_act(i, c, act):
        def one(j, d):
            @pl.when(lax.rem(d, 2) == 0)
            def _():
                act(to(ho_part(i, c), block(i, c, m), straight_send.at[i, c, j], x_recv.at[i, c, m], s + 1, j))

        others_far_first(one)

    def home(i, act):
        act(to(ho.at[:, rows_of(i), :], fin, fin_send.at[i], fin_recv, i, m))

    for i in range(S):
        def out_step(p, carry):
            j = nth(p)

            @pl.when(j != m)
            def _():
                for g in range(parts):
                    got(mix_part(i, g, j), mix_recv.at[i, g, j])
            cols = pl.ds(pl.multiple_of(j * Wl, Wl), Wl)
            update = jnp.dot(hg[i * L : (i + 1) * L, cols], wo[cols, :], preferred_element_type=jnp.float32)
            out_acc[...] = jnp.where(p == 0, update, out_acc[...] + update)
            return carry

        lax.fori_loop(0, M, out_step, 0)
        for c in range(C):
            total = xg[m, c, i * L : (i + 1) * L, :].astype(jnp.float32) + out_acc[:, c * Dc : (c + 1) * Dc]
            ho[c, i * L : (i + 1) * L, :] = total.astype(jnp.bfloat16)

            @pl.when(s < S - 1)
            def _():
                up_act(i, c, start)

        @pl.when(s < S - 1)
        def _():
            for c in range(C):
                straight_act(i, c, start)

        if i < S - 1:
            @pl.when(s == S - 1)
            def _():
                home(i, start)

    @pl.when(lax.rem(s, 2) == 0)
    def _():
        transit_all(start, True)

    @pl.when(s == 0)
    def _():
        for c in range(C):
            along(m, c, x_part(c), sent)
            others(lambda j, d: along(j, c, block(0, c, j), sent))

    @pl.when(s > 0)
    def _():
        first_out(sent)

    for i in range(S):
        for g in range(parts):
            mix_act(i, g, sent)

        @pl.when(s > 0)
        def _():
            for c in range(C):
                relay_act(i, c, sent)

        @pl.when(s < S - 1)
        def _():
            for c in range(C):
                up_act(i, c, sent)
                straight_act(i, c, sent)

        if i < S - 1:
            @pl.when(s == S - 1)
            def _():
                home(i, sent)

    transit_all(sent, False)

    @pl.when(s == S - 1)
    def _():
        for c in range(C):
            o_ref[:, c * Dc : (c + 1) * Dc] = ho[c, (S - 1) * L :, :]

    @pl.when(s < S - 1)
    def _():
        got(fin, fin_recv)
        for c in range(C):
            o_ref[:, c * Dc : (c + 1) * Dc] = fin[c]


def solution(mesh):
    S, M = mesh.shape["section"], mesh.shape["mp"]

    def shards(micro_inputs, qkv_weight, out_weight, norm_gain, position_bias):
        L, Dl = micro_inputs.shape[1:]
        D = qkv_weight.shape[1]
        Wl = qkv_weight.shape[3]
        H = position_bias.shape[0]
        R = S * L
        hs = Wl // H
        G = head_group(H, hs)
        N = H // G
        parts = N
        C = column_parts(Dl)
        buckets = jnp.asarray(bucket_table(L, position_bias.shape[1], REACH).T)
        wq = jnp.transpose(qkv_weight[0], (1, 0, 2))
        bf16, f32 = jnp.bfloat16, jnp.float32
        dma = pltpu.SemaphoreType.DMA
        vmem = pl.BlockSpec(memory_space=pltpu.VMEM)
        out = pl.pallas_call(
            functools.partial(kernel, (S, M, L, H, hs)),
            out_shape=pltpu.VMEM((L, Dl), bf16),
            in_specs=[
                vmem, vmem, vmem, pl.BlockSpec(memory_space=pltpu.SMEM),
                pl.BlockSpec(memory_space=pltpu.HBM), pl.BlockSpec(memory_space=pltpu.HBM),
            ],
            out_specs=vmem,
            scratch_shapes=[
                pltpu.VMEM((M, C, R, Dl // C), bf16),
                pltpu.VMEM((R, M * Wl), bf16),
                pltpu.VMEM((S, parts, L, Wl // parts), bf16),
                pltpu.VMEM((C, R, Dl // C), bf16),
                pltpu.VMEM((C, L, Dl // C), bf16),
                pltpu.VMEM((3, D, Wl), bf16),
                pltpu.VMEM((M * Wl, Dl), bf16),
                pltpu.VMEM((L, 3 * Wl), f32),
                pltpu.VMEM((L, Dl), f32),
                pltpu.VMEM((L, 128), f32),
                pltpu.VMEM((L, 3 * Wl), bf16),
                pltpu.VMEM((N, L, G * L), f32),
                pltpu.VMEM((G * L, G * hs), bf16),
                dma((M,)), dma,
                dma((S, C, M)), dma((C, 4, M)), dma((C, M)), dma((S, C)), dma((S, C, M)), dma((S, C, M)),
                dma((S, parts, M)), dma((S, parts, M)), dma((S, parts)), dma((S, parts)), dma((S, parts, M)),
                dma((S,)), dma,
            ],
            compiler_params=pltpu.CompilerParams(
                collective_id=0, has_side_effects=True, vmem_limit_bytes=60 * 1024 * 1024
            ),
        )(micro_inputs[0], norm_gain, buckets, position_bias, wq, out_weight[0])
        return out[None]

    in_specs = (
        P(("dp", "section"), None, "mp"),
        P("section", None, None, "mp"),
        P("section", None, "mp"),
        P("section", None),
        P("mp", None),
    )
    out_specs = P(("dp", "section"), None, "mp")
    return jax.shard_map(shards, mesh=mesh, in_specs=in_specs, out_specs=out_specs, check_vma=False)
```

```python
import functools
import math

import jax
import jax.numpy as jnp
import numpy as np
from jax import lax
from jax.experimental import pallas as pl
from jax.experimental.pallas import tpu as pltpu
from jax.sharding import PartitionSpec as P

REACH = 128
NORM_EPSILON = 0.1
MESH = pl.DeviceIdType.MESH
LAST_DETOUR = 3
EARLY = 1
NEAR = True


def bucket_table(length, bucket_count, reach_limit):
    offset = np.arange(length)[None, :] - np.arange(length)[:, None]
    half_count = bucket_count // 2
    upper_side = (offset > 0).astype(np.int32) * half_count
    distance = np.abs(offset)
    exact_count = half_count // 2
    scaled = (
        np.log(np.maximum(distance, 1) / exact_count)
        / np.log(reach_limit / exact_count)
        * (half_count - exact_count)
    )
    far_bucket = np.minimum(exact_count + scaled.astype(np.int32), half_count - 1)
    return (upper_side + np.where(distance < exact_count, distance, far_bucket)).astype(np.int32)


def head_group(heads, head_size):
    return max(g for g in range(1, heads + 1) if heads % g == 0 and g * head_size <= 256)


def column_parts(width):
    return 2 if width % 256 == 0 else 1


def kernel(
    sizes,
    x_ref, gain_ref, bucket_ref, pbias_ref, wq_hbm, wo_hbm,
    o_ref,
    pre, xg, hg, transit, ho, fin, wq, wo, acc, out_acc, sq, qkv, bias, head_mask,
    wq_sem, wo_sem,
    pre_recv, x_recv, line_send, down_send, up_send, straight_send, relay_send,
    mix_recv, mix_send, transit_recv, transit_up, transit_send,
    fin_send, fin_recv,
):
    S, M, L, H, hs = sizes
    C, _, Dc = ho.shape
    _, parts, _, Wp = transit.shape
    Dl = x_ref.shape[1]
    Wl = H * hs
    G = head_group(H, hs)
    Wg = G * hs
    D = M * Dl
    s = lax.axis_index("section")
    m = lax.axis_index("mp")

    def to(src, dst, send, recv, sec, col):
        return pltpu.make_async_remote_copy(
            src_ref=src, dst_ref=dst, send_sem=send, recv_sem=recv,
            device_id={"section": sec, "mp": col}, device_id_type=MESH,
        )

    def start(c):
        c.start()

    def sent(c):
        c.wait_send()

    def got(dst, recv):
        to(dst, dst, fin_send.at[0], recv, s, lax.rem(m + 1, M)).wait_recv()

    near = jnp.minimum(m, M - 1 - m)
    longer = jnp.where(m > M - 1 - m, -1, 1)

    def nth(p):
        k = (p + 1) // 2
        both = jnp.where(p % 2 == 1, -k, k)
        return m + jnp.where(p <= 2 * near, both, longer * (p - near))

    hand_on = jnp.where(near > 0, 3, 2) if M > 3 else 1

    def relay_first(p):
        return nth(jnp.where(p == 1, hand_on, jnp.where((p > 1) & (p <= hand_on), p - 1, p)))

    def others(body):
        def step(p, carry):
            j = nth(p)
            body(j, jnp.abs(j - m))
            return carry

        lax.fori_loop(1, M, step, 0)

    def others_far_first(body):
        def step(p, carry):
            j = nth(M - p)
            body(j, jnp.abs(j - m))
            return carry

        lax.fori_loop(1, M, step, 0)

    def wq_copy(j):
        rows = pl.ds(pl.multiple_of(j * Dl, Dl), Dl)
        return pltpu.make_async_copy(wq_hbm.at[:, rows, :], wq.at[:, rows, :], wq_sem.at[j])

    def wo_copy():
        return pltpu.make_async_copy(wo_hbm, wo, wo_sem)

    barrier = pltpu.get_barrier_semaphore()

    def greet(sec, col):
        pl.semaphore_signal(barrier, inc=1, device_id={"section": sec, "mp": col}, device_id_type=MESH)

    if NEAR and S <= 2:
        if S == 2:
            greet(1 - s, m)

        greeted = S - 1
        for reach in (1, 2):
            @pl.when(m >= reach)
            def _():
                greet(s, m - reach)

            @pl.when(m < M - reach)
            def _():
                greet(s, m + reach)

            greeted = greeted + jnp.where(m >= reach, 1, 0) + jnp.where(m < M - reach, 1, 0)
    else:
        for o in range(S):
            for k in range(M):
                if o or k:
                    greet(lax.rem(s + o, S), lax.rem(m + k, M))
        greeted = S * M - 1

    for p in range(M):
        wq_copy(nth(p)).start()
    wo_copy().start()
    pl.semaphore_wait(barrier, greeted)

    def rows_of(i):
        return pl.ds(i * L, L)

    def x_part(c):
        return x_ref.at[:, pl.ds(c * Dc, Dc)]

    def block(i, c, j):
        return xg.at[j, c, rows_of(i), :]

    def ring(c, j, src, dst, recv, act):
        even = lax.rem(m - j + 2 * M, 2) == 0
        for reach in (2, 1):
            @pl.when((j <= m) & even & (m < M - reach))
            def _():
                act(to(src, dst, line_send.at[c, reach - 1, j], recv, s, m + reach))

            @pl.when((j >= m) & even & (m >= reach))
            def _():
                act(to(src, dst, line_send.at[c, reach + 1, j], recv, s, m - reach))

    def along(c, j, src, act):
        ring(c, j, src, block(0, c, j), x_recv.at[0, c, j], act)

    def hop(c, j, src, dst, recv, act):
        @pl.when((j <= m) & (m < M - 1))
        def _():
            act(to(src, dst, line_send.at[c, 0, j], recv, s, m + 1))

        @pl.when((j >= m) & (m > 0))
        def _():
            act(to(src, dst, line_send.at[c, 1, j], recv, s, m - 1))

    def down(c, j, src, act):
        dst = xg.at[j, c, pl.ds(pl.multiple_of(s * L, L), L), :]
        act(to(src, dst, down_send.at[c, j], x_recv.at[s, c, j], 0, m))
        hop(c, j, src, pre.at[j, c], pre_recv.at[c, j], act)

    @pl.when(s == 0)
    def _():
        for c in range(C):
            along(c, m, x_part(c), start)

    @pl.when(s > 0)
    def _():
        for c in range(C):
            down(c, m, x_part(c), start)

    for g in range(H // G):
        heads = []
        for h in range(g * G, (g + 1) * G):
            total = jnp.zeros(bucket_ref.shape, jnp.float32)
            for b in range(pbias_ref.shape[1]):
                total = jnp.where(bucket_ref[...] == b, pbias_ref[h, b], total)
            heads.append(total)
        bias[g] = jnp.concatenate(heads, axis=1)
    head_mask[...] = jnp.where(
        lax.broadcasted_iota(jnp.int32, (G * L, Wg), 0) // L
        == lax.broadcasted_iota(jnp.int32, (G * L, Wg), 1) // hs,
        1.0,
        0.0,
    ).astype(jnp.bfloat16)

    @pl.when(s > 0)
    def _():
        def hand_down(c, j):
            got(pre.at[j, c], pre_recv.at[c, j])
            down(c, j, pre.at[j, c], start)

        def hand_step(d, carry):
            for c in range(C):
                @pl.when(m >= d)
                def _():
                    hand_down(c, m - d)

                @pl.when(m < M - d)
                def _():
                    hand_down(c, m + d)
            return carry

        lax.fori_loop(1, M, hand_step, 0)

    pair = s + 1 - 2 * lax.rem(s, 2)
    paired = pair < S

    def detour_from(i, row):
        return jnp.where((lax.rem(row, 2) == 1) & (i == S - 1), LAST_DETOUR, 3)

    def detoured(i, row, d):
        return paired & (d >= detour_from(i, row))

    def mix_part(i, g, j):
        return hg.at[rows_of(i), pl.ds(pl.multiple_of(j * Wl + g * Wp, Wp), Wp)]

    def far_reach(i, row):
        return paired & (jnp.maximum(m, M - 1 - m) >= detour_from(i, row))

    def mix_act(i, g, act):
        src = mix_part(i, g, m)

        @pl.when(far_reach(i, s))
        def _():
            act(to(src, transit.at[i, g], transit_up.at[i, g], transit_recv.at[i, g], pair, m))

        def one(j, d):
            @pl.when(jnp.logical_not(detoured(i, s, d)))
            def _():
                act(to(src, src, mix_send.at[i, g, j], mix_recv.at[i, g, m], s, j))

        others_far_first(one)

    def transit_act(i, g, act):
        def one(j, d):
            @pl.when(detoured(i, pair, d))
            def _():
                act(to(transit.at[i, g], mix_part(i, g, m), transit_send.at[i, g, j],
                       mix_recv.at[i, g, m], pair, j))

        others(one)

    def transit_all(act, wait):
        for i in range(S):
            @pl.when(far_reach(i, pair))
            def _():
                for g in range(parts):
                    if wait:
                        got(transit.at[i, g], transit_recv.at[i, g])
                    transit_act(i, g, act)

    def relay_act(i, c, act):
        def one(j, d):
            @pl.when(lax.rem(d, 2) == 1)
            def _():
                act(to(block(i, c, m), block(i, c, m), relay_send.at[i, c, j], x_recv.at[i, c, m], s, j))

        others_far_first(one)

    def relay(i):
        for c in range(C):
            got(block(i, c, m), x_recv.at[i, c, m])
            relay_act(i, c, start)

    @pl.when(lax.rem(s, 2) == 1)
    def _():
        transit_all(start, True)

    scale = 1.0 / math.sqrt(hs)
    lane_head = lax.broadcasted_iota(jnp.int32, (L, Wg), 1) // hs

    def attend(i):
        for g in range(H // G):
            q = qkv[:, g * Wg : (g + 1) * Wg]
            k = qkv[:, Wl + g * Wg : Wl + (g + 1) * Wg]
            v = qkv[:, 2 * Wl + g * Wg : 2 * Wl + (g + 1) * Wg]
            apart = jnp.concatenate([q] * G, axis=0) * head_mask[...]
            scores = lax.dot_general(
                k, apart, (((1,), (1,)), ((), ())), preferred_element_type=jnp.float32
            ) * scale + bias[g]
            weights = jnp.exp(scores - jnp.max(scores, axis=0, keepdims=True))
            probs = (weights / jnp.sum(weights, axis=0, keepdims=True)).astype(jnp.bfloat16)
            mixed = lax.dot_general(
                probs, v, (((0,), (0,)), ((), ())), preferred_element_type=jnp.float32
            )
            out = mixed[0:L]
            for h in range(1, G):
                out = jnp.where(lane_head == h, mixed[h * L : (h + 1) * L], out)
            cols = pl.ds(pl.multiple_of(m * Wl + g * Wg, Wg), Wg)
            hg[i * L : (i + 1) * L, cols] = out.astype(jnp.bfloat16)
            if parts > 1:
                mix_act(i, g, start)
        if parts == 1:
            mix_act(i, 0, start)

    def qkv_block(i, c, j):
        part_block = xg[j, c, i * L : (i + 1) * L, :].astype(jnp.float32)
        squares = part_block * part_block
        part = squares[:, 0:128]
        for k in range(1, Dc // 128):
            part = part + squares[:, k * 128 : (k + 1) * 128]
        sq[...] += part
        rows = pl.ds(pl.multiple_of(j * Dl + c * Dc, Dc), Dc)
        gained = (part_block * gain_ref[:, rows].astype(jnp.float32)).astype(jnp.bfloat16)
        for t in range(3):
            cols = pl.ds(t * Wl, Wl)
            acc[:, cols] += jnp.dot(gained, wq[t, rows, :], preferred_element_type=jnp.float32)

    for i in range(S):
        acc[...] = jnp.zeros_like(acc)
        sq[...] = jnp.zeros_like(sq)

        if i == 0:
            @pl.when(s == 0)
            def _():
                for c in range(C):
                    xg[m, c, 0:L, :] = x_ref[:, c * Dc : (c + 1) * Dc]

            @pl.when(s > 0)
            def _():
                relay(0)

        def qkv_step(p, carry):
            j = relay_first(p) if i == 0 else nth(p)
            if i == 0:
                wq_copy(j).wait()
            for c in range(C):
                @pl.when((j != m) | (s == 0) & (i > 0))
                def _():
                    got(block(i, c, j), x_recv.at[i, c, j])
                    if i == 0:
                        @pl.when(s == 0)
                        def _():
                            along(c, j, block(0, c, j), start)
                qkv_block(i, c, j)
            return carry

        early = min(EARLY, M)
        lax.fori_loop(0, early, qkv_step, 0)
        if i < S - 1:
            @pl.when(s > 0)
            def _():
                relay(i + 1)
        lax.fori_loop(early, M, qkv_step, 0)
        row_scale = lax.rsqrt(jnp.sum(sq[...], axis=1, keepdims=True) / D + NORM_EPSILON)
        qkv[...] = (acc[...] * row_scale).astype(jnp.bfloat16)
        attend(i)

    wo_copy().wait()

    def ho_part(i, c):
        return ho.at[c, rows_of(i), :]

    def up_act(i, c, act):
        act(to(ho_part(i, c), block(i, c, m), up_send.at[i, c], x_recv.at[i, c, m], s + 1, m))

    def straight_act(i, c, act):
        def one(j, d):
            @pl.when(lax.rem(d, 2) == 0)
            def _():
                act(to(ho_part(i, c), block(i, c, m), straight_send.at[i, c, j], x_recv.at[i, c, m], s + 1, j))

        others_far_first(one)

    def home(i, act):
        act(to(ho.at[:, rows_of(i), :], fin, fin_send.at[i], fin_recv, i, m))

    for i in range(S):
        def out_step(p, carry):
            j = nth(p)

            @pl.when(j != m)
            def _():
                for g in range(parts):
                    got(mix_part(i, g, j), mix_recv.at[i, g, j])
            cols = pl.ds(pl.multiple_of(j * Wl, Wl), Wl)
            update = jnp.dot(hg[i * L : (i + 1) * L, cols], wo[cols, :], preferred_element_type=jnp.float32)
            out_acc[...] = jnp.where(p == 0, update, out_acc[...] + update)
            return carry

        lax.fori_loop(0, M, out_step, 0)
        for c in range(C):
            total = xg[m, c, i * L : (i + 1) * L, :].astype(jnp.float32) + out_acc[:, c * Dc : (c + 1) * Dc]
            ho[c, i * L : (i + 1) * L, :] = total.astype(jnp.bfloat16)

            @pl.when(s < S - 1)
            def _():
                up_act(i, c, start)

        @pl.when(s < S - 1)
        def _():
            for c in range(C):
                straight_act(i, c, start)

        if i < S - 1:
            @pl.when(s == S - 1)
            def _():
                home(i, start)

    @pl.when(lax.rem(s, 2) == 0)
    def _():
        transit_all(start, True)

    @pl.when(s == 0)
    def _():
        for c in range(C):
            along(c, m, x_part(c), sent)
            others(lambda j, d: along(c, j, block(0, c, j), sent))

    @pl.when(s > 0)
    def _():
        for c in range(C):
            down(c, m, x_part(c), sent)
            others(lambda j, d: down(c, j, pre.at[j, c], sent))

    for i in range(S):
        for g in range(parts):
            mix_act(i, g, sent)

        @pl.when(s > 0)
        def _():
            for c in range(C):
                relay_act(i, c, sent)

        @pl.when(s < S - 1)
        def _():
            for c in range(C):
                up_act(i, c, sent)
                straight_act(i, c, sent)

        if i < S - 1:
            @pl.when(s == S - 1)
            def _():
                home(i, sent)

    transit_all(sent, False)

    @pl.when(s == S - 1)
    def _():
        for c in range(C):
            o_ref[:, c * Dc : (c + 1) * Dc] = ho[c, (S - 1) * L :, :]

    @pl.when(s < S - 1)
    def _():
        got(fin, fin_recv)
        for c in range(C):
            o_ref[:, c * Dc : (c + 1) * Dc] = fin[c]


def solution(mesh):
    S, M = mesh.shape["section"], mesh.shape["mp"]

    def shards(micro_inputs, qkv_weight, out_weight, norm_gain, position_bias):
        L, Dl = micro_inputs.shape[1:]
        D = qkv_weight.shape[1]
        Wl = qkv_weight.shape[3]
        H = position_bias.shape[0]
        R = S * L
        hs = Wl // H
        G = head_group(H, hs)
        N = H // G
        parts = N
        C = column_parts(Dl)
        buckets = jnp.asarray(bucket_table(L, position_bias.shape[1], REACH).T)
        wq = jnp.transpose(qkv_weight[0], (1, 0, 2))
        bf16, f32 = jnp.bfloat16, jnp.float32
        dma = pltpu.SemaphoreType.DMA
        vmem = pl.BlockSpec(memory_space=pltpu.VMEM)
        out = pl.pallas_call(
            functools.partial(kernel, (S, M, L, H, hs)),
            out_shape=pltpu.VMEM((L, Dl), bf16),
            in_specs=[
                vmem, vmem, vmem, pl.BlockSpec(memory_space=pltpu.SMEM),
                pl.BlockSpec(memory_space=pltpu.HBM), pl.BlockSpec(memory_space=pltpu.HBM),
            ],
            out_specs=vmem,
            scratch_shapes=[
                pltpu.VMEM((M, C, L, Dl // C), bf16),
                pltpu.VMEM((M, C, R, Dl // C), bf16),
                pltpu.VMEM((R, M * Wl), bf16),
                pltpu.VMEM((S, parts, L, Wl // parts), bf16),
                pltpu.VMEM((C, R, Dl // C), bf16),
                pltpu.VMEM((C, L, Dl // C), bf16),
                pltpu.VMEM((3, D, Wl), bf16),
                pltpu.VMEM((M * Wl, Dl), bf16),
                pltpu.VMEM((L, 3 * Wl), f32),
                pltpu.VMEM((L, Dl), f32),
                pltpu.VMEM((L, 128), f32),
                pltpu.VMEM((L, 3 * Wl), bf16),
                pltpu.VMEM((N, L, G * L), f32),
                pltpu.VMEM((G * L, G * hs), bf16),
                dma((M,)), dma,
                dma((C, M)), dma((S, C, M)), dma((C, 4, M)), dma((C, M)), dma((S, C)), dma((S, C, M)), dma((S, C, M)),
                dma((S, parts, M)), dma((S, parts, M)), dma((S, parts)), dma((S, parts)), dma((S, parts, M)),
                dma((S,)), dma,
            ],
            compiler_params=pltpu.CompilerParams(
                collective_id=0, has_side_effects=True, vmem_limit_bytes=60 * 1024 * 1024
            ),
        )(micro_inputs[0], norm_gain, buckets, position_bias, wq, out_weight[0])
        return out[None]

    in_specs = (
        P(("dp", "section"), None, "mp"),
        P("section", None, None, "mp"),
        P("section", None, "mp"),
        P("section", None),
        P("mp", None),
    )
    out_specs = P(("dp", "section"), None, "mp")
    return jax.shard_map(shards, mesh=mesh, in_specs=in_specs, out_specs=out_specs, check_vma=False)
```

```python
import functools
import math

import jax
import jax.numpy as jnp
import numpy as np
from jax import lax
from jax.experimental import pallas as pl
from jax.experimental.pallas import tpu as pltpu
from jax.sharding import PartitionSpec as P

REACH = 128
NORM_EPSILON = 0.1
MESH = pl.DeviceIdType.MESH
LAST_DETOUR = 3
EARLY = 1
NEAR = True


def bucket_table(length, bucket_count, reach_limit):
    offset = np.arange(length)[None, :] - np.arange(length)[:, None]
    half_count = bucket_count // 2
    upper_side = (offset > 0).astype(np.int32) * half_count
    distance = np.abs(offset)
    exact_count = half_count // 2
    scaled = (
        np.log(np.maximum(distance, 1) / exact_count)
        / np.log(reach_limit / exact_count)
        * (half_count - exact_count)
    )
    far_bucket = np.minimum(exact_count + scaled.astype(np.int32), half_count - 1)
    return (upper_side + np.where(distance < exact_count, distance, far_bucket)).astype(np.int32)


def head_group(heads, head_size):
    return max(g for g in range(1, heads + 1) if heads % g == 0 and g * head_size <= 256)


def column_parts(width):
    return 2 if width % 256 == 0 else 1


def kernel(
    sizes,
    x_ref, gain_ref, bucket_ref, pbias_ref, wq_hbm, wo_hbm,
    o_ref,
    pre, xg, hg, transit, ho, fin, wq, wo, acc, out_acc, sq, qkv, bias, head_mask,
    wq_sem, wo_sem,
    pre_recv, x_recv, line_send, down_send, up_send, straight_send, relay_send,
    mix_recv, mix_send, transit_recv, transit_up, transit_send,
    fin_send, fin_recv,
):
    S, M, L, H, hs = sizes
    C, _, Dc = ho.shape
    _, parts, _, Wp = transit.shape
    Dl = x_ref.shape[1]
    Wl = H * hs
    G = head_group(H, hs)
    Wg = G * hs
    D = M * Dl
    s = lax.axis_index("section")
    m = lax.axis_index("mp")

    def to(src, dst, send, recv, sec, col):
        return pltpu.make_async_remote_copy(
            src_ref=src, dst_ref=dst, send_sem=send, recv_sem=recv,
            device_id={"section": sec, "mp": col}, device_id_type=MESH,
        )

    def start(c):
        c.start()

    def sent(c):
        c.wait_send()

    def got(dst, recv):
        to(dst, dst, fin_send.at[0, 0], recv, s, lax.rem(m + 1, M)).wait_recv()

    near = jnp.minimum(m, M - 1 - m)
    longer = jnp.where(m > M - 1 - m, -1, 1)

    def nth(p):
        k = (p + 1) // 2
        both = jnp.where(p % 2 == 1, -k, k)
        return m + jnp.where(p <= 2 * near, both, longer * (p - near))

    hand_on = jnp.where(near > 0, 3, 2) if M > 3 else 1

    def relay_first(p):
        return nth(jnp.where(p == 1, hand_on, jnp.where((p > 1) & (p <= hand_on), p - 1, p)))

    def others(body):
        def step(p, carry):
            j = nth(p)
            body(j, jnp.abs(j - m))
            return carry

        lax.fori_loop(1, M, step, 0)

    def others_far_first(body):
        def step(p, carry):
            j = nth(M - p)
            body(j, jnp.abs(j - m))
            return carry

        lax.fori_loop(1, M, step, 0)

    def wq_copy(j):
        rows = pl.ds(pl.multiple_of(j * Dl, Dl), Dl)
        return pltpu.make_async_copy(wq_hbm.at[:, rows, :], wq.at[:, rows, :], wq_sem.at[j])

    def wo_copy():
        return pltpu.make_async_copy(wo_hbm, wo, wo_sem)

    barrier = pltpu.get_barrier_semaphore()

    def greet(sec, col):
        pl.semaphore_signal(barrier, inc=1, device_id={"section": sec, "mp": col}, device_id_type=MESH)

    if NEAR and S <= 2:
        if S == 2:
            greet(1 - s, m)

        greeted = S - 1
        for reach in (1, 2):
            @pl.when(m >= reach)
            def _():
                greet(s, m - reach)

            @pl.when(m < M - reach)
            def _():
                greet(s, m + reach)

            greeted = greeted + jnp.where(m >= reach, 1, 0) + jnp.where(m < M - reach, 1, 0)
    else:
        for o in range(S):
            for k in range(M):
                if o or k:
                    greet(lax.rem(s + o, S), lax.rem(m + k, M))
        greeted = S * M - 1

    for p in range(M):
        wq_copy(nth(p)).start()
    wo_copy().start()
    pl.semaphore_wait(barrier, greeted)

    def rows_of(i):
        return pl.ds(i * L, L)

    def x_part(c):
        return x_ref.at[:, pl.ds(c * Dc, Dc)]

    def block(i, c, j):
        return xg.at[j, c, rows_of(i), :]

    def ring(c, j, src, dst, recv, act):
        even = lax.rem(m - j + 2 * M, 2) == 0
        for reach in (2, 1):
            @pl.when((j <= m) & even & (m < M - reach))
            def _():
                act(to(src, dst, line_send.at[c, reach - 1, j], recv, s, m + reach))

            @pl.when((j >= m) & even & (m >= reach))
            def _():
                act(to(src, dst, line_send.at[c, reach + 1, j], recv, s, m - reach))

    def along(c, j, src, act):
        ring(c, j, src, block(0, c, j), x_recv.at[0, c, j], act)

    def hop(c, j, src, dst, recv, act):
        @pl.when((j <= m) & (m < M - 1))
        def _():
            act(to(src, dst, line_send.at[c, 0, j], recv, s, m + 1))

        @pl.when((j >= m) & (m > 0))
        def _():
            act(to(src, dst, line_send.at[c, 1, j], recv, s, m - 1))

    def down(c, j, src, act):
        dst = xg.at[j, c, pl.ds(pl.multiple_of(s * L, L), L), :]
        act(to(src, dst, down_send.at[c, j], x_recv.at[s, c, j], 0, m))
        hop(c, j, src, pre.at[j, c], pre_recv.at[c, j], act)

    @pl.when(s == 0)
    def _():
        for c in range(C):
            along(c, m, x_part(c), start)

    @pl.when(s > 0)
    def _():
        for c in range(C):
            down(c, m, x_part(c), start)

    for g in range(H // G):
        heads = []
        for h in range(g * G, (g + 1) * G):
            total = jnp.zeros(bucket_ref.shape, jnp.float32)
            for b in range(pbias_ref.shape[1]):
                total = jnp.where(bucket_ref[...] == b, pbias_ref[h, b], total)
            heads.append(total)
        bias[g] = jnp.concatenate(heads, axis=1)
    head_mask[...] = jnp.where(
        lax.broadcasted_iota(jnp.int32, (G * L, Wg), 0) // L
        == lax.broadcasted_iota(jnp.int32, (G * L, Wg), 1) // hs,
        1.0,
        0.0,
    ).astype(jnp.bfloat16)

    @pl.when(s > 0)
    def _():
        def hand_down(c, j):
            got(pre.at[j, c], pre_recv.at[c, j])
            down(c, j, pre.at[j, c], start)

        def hand_step(d, carry):
            for c in range(C):
                @pl.when(m >= d)
                def _():
                    hand_down(c, m - d)

                @pl.when(m < M - d)
                def _():
                    hand_down(c, m + d)
            return carry

        lax.fori_loop(1, M, hand_step, 0)

    pair = s + 1 - 2 * lax.rem(s, 2)
    paired = pair < S

    def detour_from(i, row):
        return jnp.where((lax.rem(row, 2) == 1) & (i == S - 1), LAST_DETOUR, 3)

    def detoured(i, row, d):
        return paired & (d >= detour_from(i, row))

    def mix_part(i, g, j):
        return hg.at[rows_of(i), pl.ds(pl.multiple_of(j * Wl + g * Wp, Wp), Wp)]

    def far_reach(i, row):
        return paired & (jnp.maximum(m, M - 1 - m) >= detour_from(i, row))

    def mix_act(i, g, act):
        src = mix_part(i, g, m)

        @pl.when(far_reach(i, s))
        def _():
            act(to(src, transit.at[i, g], transit_up.at[i, g], transit_recv.at[i, g], pair, m))

        def one(j, d):
            @pl.when(jnp.logical_not(detoured(i, s, d)))
            def _():
                act(to(src, src, mix_send.at[i, g, j], mix_recv.at[i, g, m], s, j))

        others_far_first(one)

    def transit_act(i, g, act):
        def one(j, d):
            @pl.when(detoured(i, pair, d))
            def _():
                act(to(transit.at[i, g], mix_part(i, g, m), transit_send.at[i, g, j],
                       mix_recv.at[i, g, m], pair, j))

        others(one)

    def transit_all(act, wait):
        for i in range(S):
            @pl.when(far_reach(i, pair))
            def _():
                for g in range(parts):
                    if wait:
                        got(transit.at[i, g], transit_recv.at[i, g])
                    transit_act(i, g, act)

    def relay_act(i, c, act):
        def one(j, d):
            @pl.when(lax.rem(d, 2) == 1)
            def _():
                act(to(block(i, c, m), block(i, c, m), relay_send.at[i, c, j], x_recv.at[i, c, m], s, j))

        others_far_first(one)

    def relay(i):
        for c in range(C):
            got(block(i, c, m), x_recv.at[i, c, m])
            relay_act(i, c, start)

    @pl.when(lax.rem(s, 2) == 1)
    def _():
        transit_all(start, True)

    scale = 1.0 / math.sqrt(hs)
    lane_head = lax.broadcasted_iota(jnp.int32, (L, Wg), 1) // hs

    def attend(i):
        for g in range(H // G):
            q = qkv[:, g * Wg : (g + 1) * Wg]
            k = qkv[:, Wl + g * Wg : Wl + (g + 1) * Wg]
            v = qkv[:, 2 * Wl + g * Wg : 2 * Wl + (g + 1) * Wg]
            apart = jnp.concatenate([q] * G, axis=0) * head_mask[...]
            scores = lax.dot_general(
                k, apart, (((1,), (1,)), ((), ())), preferred_element_type=jnp.float32
            ) * scale + bias[g]
            weights = jnp.exp(scores - jnp.max(scores, axis=0, keepdims=True))
            probs = (weights / jnp.sum(weights, axis=0, keepdims=True)).astype(jnp.bfloat16)
            mixed = lax.dot_general(
                probs, v, (((0,), (0,)), ((), ())), preferred_element_type=jnp.float32
            )
            out = mixed[0:L]
            for h in range(1, G):
                out = jnp.where(lane_head == h, mixed[h * L : (h + 1) * L], out)
            cols = pl.ds(pl.multiple_of(m * Wl + g * Wg, Wg), Wg)
            hg[i * L : (i + 1) * L, cols] = out.astype(jnp.bfloat16)
            if parts > 1:
                mix_act(i, g, start)
        if parts == 1:
            mix_act(i, 0, start)

    def qkv_block(i, c, j):
        part_block = xg[j, c, i * L : (i + 1) * L, :].astype(jnp.float32)
        squares = part_block * part_block
        part = squares[:, 0:128]
        for k in range(1, Dc // 128):
            part = part + squares[:, k * 128 : (k + 1) * 128]
        sq[...] += part
        rows = pl.ds(pl.multiple_of(j * Dl + c * Dc, Dc), Dc)
        gained = (part_block * gain_ref[:, rows].astype(jnp.float32)).astype(jnp.bfloat16)
        for t in range(3):
            cols = pl.ds(t * Wl, Wl)
            acc[:, cols] += jnp.dot(gained, wq[t, rows, :], preferred_element_type=jnp.float32)

    for i in range(S):
        acc[...] = jnp.zeros_like(acc)
        sq[...] = jnp.zeros_like(sq)

        if i == 0:
            @pl.when(s == 0)
            def _():
                for c in range(C):
                    xg[m, c, 0:L, :] = x_ref[:, c * Dc : (c + 1) * Dc]

            @pl.when(s > 0)
            def _():
                relay(0)

        def qkv_step(p, carry):
            j = relay_first(p) if i == 0 else nth(p)
            if i == 0:
                wq_copy(j).wait()
            for c in range(C):
                @pl.when((j != m) | (s == 0) & (i > 0))
                def _():
                    got(block(i, c, j), x_recv.at[i, c, j])
                    if i == 0:
                        @pl.when(s == 0)
                        def _():
                            along(c, j, block(0, c, j), start)
                qkv_block(i, c, j)
            return carry

        early = min(EARLY, M)
        lax.fori_loop(0, early, qkv_step, 0)
        if i < S - 1:
            @pl.when(s > 0)
            def _():
                relay(i + 1)
        lax.fori_loop(early, M, qkv_step, 0)
        row_scale = lax.rsqrt(jnp.sum(sq[...], axis=1, keepdims=True) / D + NORM_EPSILON)
        qkv[...] = (acc[...] * row_scale).astype(jnp.bfloat16)
        attend(i)

    wo_copy().wait()

    def ho_part(i, c):
        return ho.at[c, rows_of(i), :]

    def up_act(i, c, act):
        act(to(ho_part(i, c), block(i, c, m), up_send.at[i, c], x_recv.at[i, c, m], s + 1, m))

    def straight_act(i, c, act):
        def one(j, d):
            @pl.when(lax.rem(d, 2) == 0)
            def _():
                act(to(ho_part(i, c), block(i, c, m), straight_send.at[i, c, j], x_recv.at[i, c, m], s + 1, j))

        others_far_first(one)

    def home(i, c, act):
        act(to(ho.at[c, rows_of(i), :], fin.at[c], fin_send.at[i, c], fin_recv.at[c], i, m))

    for i in range(S):
        def out_step(p, carry):
            j = nth(p)

            @pl.when(j != m)
            def _():
                for g in range(parts):
                    got(mix_part(i, g, j), mix_recv.at[i, g, j])
            cols = pl.ds(pl.multiple_of(j * Wl, Wl), Wl)
            update = jnp.dot(hg[i * L : (i + 1) * L, cols], wo[cols, :], preferred_element_type=jnp.float32)
            out_acc[...] = jnp.where(p == 0, update, out_acc[...] + update)
            return carry

        lax.fori_loop(0, M, out_step, 0)
        for c in range(C):
            total = xg[m, c, i * L : (i + 1) * L, :].astype(jnp.float32) + out_acc[:, c * Dc : (c + 1) * Dc]
            ho[c, i * L : (i + 1) * L, :] = total.astype(jnp.bfloat16)

            @pl.when(s < S - 1)
            def _():
                up_act(i, c, start)

            if i < S - 1:
                @pl.when(s == S - 1)
                def _():
                    home(i, c, start)

        @pl.when(s < S - 1)
        def _():
            for c in range(C):
                straight_act(i, c, start)

    @pl.when(lax.rem(s, 2) == 0)
    def _():
        transit_all(start, True)

    @pl.when(s == 0)
    def _():
        for c in range(C):
            along(c, m, x_part(c), sent)
            others(lambda j, d: along(c, j, block(0, c, j), sent))

    @pl.when(s > 0)
    def _():
        for c in range(C):
            down(c, m, x_part(c), sent)
            others(lambda j, d: down(c, j, pre.at[j, c], sent))

    for i in range(S):
        for g in range(parts):
            mix_act(i, g, sent)

        @pl.when(s > 0)
        def _():
            for c in range(C):
                relay_act(i, c, sent)

        @pl.when(s < S - 1)
        def _():
            for c in range(C):
                up_act(i, c, sent)
                straight_act(i, c, sent)

        if i < S - 1:
            @pl.when(s == S - 1)
            def _():
                for c in range(C):
                    home(i, c, sent)

    transit_all(sent, False)

    @pl.when(s == S - 1)
    def _():
        for c in range(C):
            o_ref[:, c * Dc : (c + 1) * Dc] = ho[c, (S - 1) * L :, :]

    @pl.when(s < S - 1)
    def _():
        for c in range(C):
            got(fin.at[c], fin_recv.at[c])
            o_ref[:, c * Dc : (c + 1) * Dc] = fin[c]


def solution(mesh):
    S, M = mesh.shape["section"], mesh.shape["mp"]

    def shards(micro_inputs, qkv_weight, out_weight, norm_gain, position_bias):
        L, Dl = micro_inputs.shape[1:]
        D = qkv_weight.shape[1]
        Wl = qkv_weight.shape[3]
        H = position_bias.shape[0]
        R = S * L
        hs = Wl // H
        G = head_group(H, hs)
        N = H // G
        parts = N
        C = column_parts(Dl)
        buckets = jnp.asarray(bucket_table(L, position_bias.shape[1], REACH).T)
        wq = jnp.transpose(qkv_weight[0], (1, 0, 2))
        bf16, f32 = jnp.bfloat16, jnp.float32
        dma = pltpu.SemaphoreType.DMA
        vmem = pl.BlockSpec(memory_space=pltpu.VMEM)
        out = pl.pallas_call(
            functools.partial(kernel, (S, M, L, H, hs)),
            out_shape=pltpu.VMEM((L, Dl), bf16),
            in_specs=[
                vmem, vmem, vmem, pl.BlockSpec(memory_space=pltpu.SMEM),
                pl.BlockSpec(memory_space=pltpu.HBM), pl.BlockSpec(memory_space=pltpu.HBM),
            ],
            out_specs=vmem,
            scratch_shapes=[
                pltpu.VMEM((M, C, L, Dl // C), bf16),
                pltpu.VMEM((M, C, R, Dl // C), bf16),
                pltpu.VMEM((R, M * Wl), bf16),
                pltpu.VMEM((S, parts, L, Wl // parts), bf16),
                pltpu.VMEM((C, R, Dl // C), bf16),
                pltpu.VMEM((C, L, Dl // C), bf16),
                pltpu.VMEM((3, D, Wl), bf16),
                pltpu.VMEM((M * Wl, Dl), bf16),
                pltpu.VMEM((L, 3 * Wl), f32),
                pltpu.VMEM((L, Dl), f32),
                pltpu.VMEM((L, 128), f32),
                pltpu.VMEM((L, 3 * Wl), bf16),
                pltpu.VMEM((N, L, G * L), f32),
                pltpu.VMEM((G * L, G * hs), bf16),
                dma((M,)), dma,
                dma((C, M)), dma((S, C, M)), dma((C, 4, M)), dma((C, M)), dma((S, C)), dma((S, C, M)), dma((S, C, M)),
                dma((S, parts, M)), dma((S, parts, M)), dma((S, parts)), dma((S, parts)), dma((S, parts, M)),
                dma((S, C)), dma((C,)),
            ],
            compiler_params=pltpu.CompilerParams(
                collective_id=0, has_side_effects=True, vmem_limit_bytes=60 * 1024 * 1024
            ),
        )(micro_inputs[0], norm_gain, buckets, position_bias, wq, out_weight[0])
        return out[None]

    in_specs = (
        P(("dp", "section"), None, "mp"),
        P("section", None, None, "mp"),
        P("section", None, "mp"),
        P("section", None),
        P("mp", None),
    )
    out_specs = P(("dp", "section"), None, "mp")
    return jax.shard_map(shards, mesh=mesh, in_specs=in_specs, out_specs=out_specs, check_vma=False)
```
